16 devices in a mesh: data: 16 (over z, y, x, core).
Axes of the slice: x: 2, y: 2, z: 2, core: 2. Of those that a mesh axis runs over, the one named last changes fastest.
Arguments:
- x_in: bfloat16 [32, 1024, 1024], P('data')
- dy_out: bfloat16 [32, 1024, 1024], P('data')
- lengths: int32 [32], P('data')
- w_one: bfloat16 [4, 1024, 4096], replicated
- w_two: bfloat16 [4, 4096, 1024], replicated
- noise_one: float32 [4, 1024, 4096], replicated
- noise_two: float32 [4, 4096, 1024], replicated
- clip_norm: float32 [1], replicated
Outputs:
- output 1: float32 [4, 1024, 4096], replicated
- output 2: float32 [4, 4096, 1024], replicated
All inputs are finite; a program needn't handle non-finite values.
Results may differ from the reference program's by a relative error of at most 0.0131301.
Values are sent between devices in bfloat16 or wider.
A program may use at most 1.5 GiB of HBM per device.

```python
import jax
import jax.numpy as jnp
from jax import lax

WIDTH = 1024
SEQ = 1024
LAYERS = 4
SAMPLES_DEV = 2
DEVICES = 16
HIDDEN = 4 * WIDTH
MICRO = SAMPLES_DEV // 2
BATCH = DEVICES * SAMPLES_DEV


def setup_inputs(seed: int = 0) -> dict:
    key_list = jax.random.split(jax.random.key(seed), 11)
    len_draw = jax.random.randint(key_list[0], (BATCH,), SEQ // 4, SEQ + 1)
    lead_sample = (jnp.arange(BATCH) % SAMPLES_DEV) == 0
    lengths = jnp.where(lead_sample, SEQ, len_draw).astype(jnp.int32)
    clipped = jax.random.bernoulli(key_list[1], 0.5, (BATCH,))
    big_scale = jax.random.uniform(key_list[2], (BATCH,), jnp.float32, 1.0, 1.8)
    small_scale = jax.random.uniform(key_list[3], (BATCH,), jnp.float32, 0.2, 0.45)
    sample_scale = jnp.where(clipped, big_scale, small_scale) * 2.0 * jnp.sqrt(BATCH / lengths.astype(jnp.float32))
    dy_out = (jax.random.normal(key_list[4], (BATCH, SEQ, WIDTH), jnp.float32) * sample_scale[:, None, None]).astype(jnp.bfloat16)
    x_in = jax.random.normal(key_list[5], (BATCH, SEQ, WIDTH), jnp.float32).astype(jnp.bfloat16)
    w_one = (jax.random.normal(key_list[6], (LAYERS, WIDTH, HIDDEN), jnp.float32) * WIDTH ** -0.5).astype(jnp.bfloat16)
    w_two = (jax.random.normal(key_list[7], (LAYERS, HIDDEN, WIDTH), jnp.float32) * (HIDDEN * LAYERS) ** -0.5).astype(jnp.bfloat16)
    noise_one = jax.random.normal(key_list[8], (LAYERS, WIDTH, HIDDEN), jnp.float32) * (0.2 * BATCH / LAYERS ** 0.5)
    noise_two = jax.random.normal(key_list[9], (LAYERS, HIDDEN, WIDTH), jnp.float32) * (0.4 * BATCH)
    clip_norm = jax.random.uniform(key_list[10], (1,), jnp.float32, 0.9, 1.1) * (2.0 * WIDTH * (LAYERS * BATCH) ** 0.5)
    return {'x_in': x_in, 'dy_out': dy_out, 'lengths': lengths, 'w_one': w_one, 'w_two': w_two, 'noise_one': noise_one, 'noise_two': noise_two, 'clip_norm': clip_norm}


def sample_gram(row_data):
    sample_mats = row_data.reshape(MICRO, SEQ, -1).astype(jnp.float32)
    return jnp.einsum('mtd,msd->mts', sample_mats, sample_mats)


def forward_stack(x_rows, w_one, w_two):
    def layer_step(x_cur, weights):
        w_up, w_down = weights
        pre_act = jnp.dot(x_cur, w_up, preferred_element_type=jnp.float32).astype(jnp.bfloat16)
        act_out = jax.nn.gelu(pre_act.astype(jnp.float32)).astype(jnp.bfloat16)
        branch = jnp.dot(act_out, w_down, preferred_element_type=jnp.float32)
        x_next = (x_cur.astype(jnp.float32) + branch).astype(jnp.bfloat16)
        return x_next, (x_cur, pre_act, act_out)
    _, saved_acts = lax.scan(layer_step, x_rows, (w_one, w_two))
    return saved_acts


def backward_stack(dy_rows, x_saved, pre_saved, act_saved, w_one, w_two):
    def layer_step(dy_cur, layer_items):
        x_cur, pre_act, act_out, w_up, w_down = layer_items
        d_act = jnp.dot(dy_cur, w_down.T, preferred_element_type=jnp.float32)
        _, gelu_back = jax.vjp(jax.nn.gelu, pre_act.astype(jnp.float32))
        d_pre = gelu_back(d_act)[0].astype(jnp.bfloat16)
        d_in = (dy_cur.astype(jnp.float32) + jnp.dot(d_pre, w_up.T, preferred_element_type=jnp.float32)).astype(jnp.bfloat16)
        norm_one = jnp.sum(sample_gram(x_cur) * sample_gram(d_pre), axis=(1, 2))
        norm_two = jnp.sum(sample_gram(act_out) * sample_gram(dy_cur), axis=(1, 2))
        return d_in, (d_pre, dy_cur, norm_one + norm_two)
    _, grad_items = lax.scan(layer_step, dy_rows, (x_saved, pre_saved, act_saved, w_one, w_two), reverse=True)
    return grad_items


def microbatch_sums(x_mb, dy_mb, len_mb, w_one, w_two, clip_norm):
    x_rows = x_mb.reshape(MICRO * SEQ, WIDTH)
    keep_mask = jnp.arange(SEQ)[None, :] < len_mb[:, None]
    dy_rows = jnp.where(keep_mask[:, :, None], dy_mb, jnp.zeros_like(dy_mb)).reshape(MICRO * SEQ, WIDTH)
    x_saved, pre_saved, act_saved = forward_stack(x_rows, w_one, w_two)
    dpre_saved, dy_saved, layer_norms = backward_stack(dy_rows, x_saved, pre_saved, act_saved, w_one, w_two)
    total_norm = jnp.sum(layer_norms, axis=0)
    factor = jnp.minimum(1.0, clip_norm[0] / jnp.sqrt(total_norm))
    row_factor = jnp.repeat(factor, SEQ)[:, None]
    contract_dims = (((0,), (0,)), ((), ()))

    def layer_gemm(layer_items):
        x_cur, act_out, d_pre, dy_cur = layer_items
        scaled_pre = (d_pre.astype(jnp.float32) * row_factor).astype(jnp.bfloat16)
        scaled_dy = (dy_cur.astype(jnp.float32) * row_factor).astype(jnp.bfloat16)
        grad_in = lax.dot_general(x_cur, scaled_pre, contract_dims, preferred_element_type=jnp.float32)
        grad_out = lax.dot_general(act_out, scaled_dy, contract_dims, preferred_element_type=jnp.float32)
        return grad_in, grad_out
    return lax.map(layer_gemm, (x_saved, act_saved, dpre_saved, dy_saved))


def reference(x_in, dy_out, lengths, w_one, w_two, noise_one, noise_two, clip_norm):
    x_dev = x_in.reshape(DEVICES, 2, MICRO, SEQ, WIDTH)
    dy_dev = dy_out.reshape(DEVICES, 2, MICRO, SEQ, WIDTH)
    len_dev = lengths.reshape(DEVICES, 2, MICRO)

    def device_step(acc_pair, dev_items):
        acc_one, acc_two = acc_pair
        x_pair, dy_pair, len_pair = dev_items
        first_one, first_two = microbatch_sums(x_pair[0], dy_pair[0], len_pair[0], w_one, w_two, clip_norm)
        second_one, second_two = microbatch_sums(x_pair[1], dy_pair[1], len_pair[1], w_one, w_two, clip_norm)
        part_one = (first_one + second_one).astype(jnp.bfloat16).astype(jnp.float32)
        part_two = (first_two + second_two).astype(jnp.bfloat16).astype(jnp.float32)
        return (acc_one + part_one, acc_two + part_two), None

    start_pair = (jnp.zeros_like(noise_one), jnp.zeros_like(noise_two))
    (sum_one, sum_two), _ = lax.scan(device_step, start_pair, (x_dev, dy_dev, len_dev))
    return (sum_one + noise_one) / BATCH, (sum_two + noise_two) / BATCH
```

```python
import functools

import jax
import jax.numpy as jnp
from jax import lax
from jax.experimental import pallas as pl
from jax.experimental.pallas import tpu as pltpu
from jax.sharding import PartitionSpec as P

BF16 = jnp.bfloat16
F32 = jnp.float32
VMEM_LIMIT = 66_000_000
C0 = 0.7978845608028654
C1 = 0.044715
NT = (((1,), (1,)), ((), ()))


def gelu_tanh(x):
    half = 0.5 * x
    return half + half * jnp.tanh(x * (C0 + (C0 * C1) * (x * x)))


def gelu_tanh_grad(x):
    sq = x * x
    t = jnp.tanh(x * (C0 + (C0 * C1) * sq))
    return (1.0 + t) * (0.5 + (x * (0.5 * C0 + (1.5 * C0 * C1) * sq)) * (1.0 - t))


def params(dims):
    return pltpu.CompilerParams(vmem_limit_bytes=VMEM_LIMIT, dimension_semantics=("arbitrary",) * dims)


def forward_kernel(tm, sub, x_ref, w1_ref, w2_ref, xs_ref, h_ref, a_ref, xcur):
    layer, m = pl.program_id(0), pl.program_id(1)
    last = pl.num_programs(0) - 1
    rows = pl.ds(pl.multiple_of(m * tm, tm), tm)

    def up():
        xs_ref[0] = jnp.where(layer == 0, x_ref[...], xcur[rows, :])
        for s in range(w1_ref.shape[-1] // sub):
            cols = slice(s * sub, (s + 1) * sub)
            h = jnp.dot(xs_ref[0], w1_ref[0, :, cols], preferred_element_type=F32).astype(BF16)
            h_ref[0, :, cols] = h
            a_ref[0, :, cols] = gelu_tanh(h.astype(F32)).astype(BF16)

    @pl.when(layer < last)
    def _():
        up()
        for s in range(w2_ref.shape[-1] // sub):
            cols = slice(s * sub, (s + 1) * sub)
            branch = jnp.dot(a_ref[0], w2_ref[0, :, cols], preferred_element_type=F32)
            xcur[rows, cols] = (xs_ref[0, :, cols].astype(F32) + branch).astype(BF16)

    @pl.when(layer == last)
    def _():
        up()


def forward_stack(x, w1, w2, tm=512, sub=512):
    layers, dm, df = w1.shape
    m_rows = x.shape[0]
    nm = m_rows // tm
    return pl.pallas_call(
        functools.partial(forward_kernel, tm, sub),
        grid=(layers, nm),
        in_specs=[
            pl.BlockSpec((tm, dm), lambda l, m: (jnp.where(l == 0, m, nm - 1), 0)),
            pl.BlockSpec((1, dm, df), lambda l, m: (l, 0, 0)),
            pl.BlockSpec((1, df, dm), lambda l, m: (jnp.minimum(l, layers - 2), 0, 0)),
        ],
        out_specs=[
            pl.BlockSpec((1, tm, dm), lambda l, m: (l, m, 0)),
            pl.BlockSpec((1, tm, df), lambda l, m: (l, m, 0)),
            pl.BlockSpec((1, tm, df), lambda l, m: (l, m, 0)),
        ],
        out_shape=[
            jax.ShapeDtypeStruct((layers, m_rows, dm), BF16),
            jax.ShapeDtypeStruct((layers, m_rows, df), BF16),
            jax.ShapeDtypeStruct((layers, m_rows, df), BF16),
        ],
        scratch_shapes=[pltpu.VMEM((m_rows, dm), BF16)],
        compiler_params=params(2),
        name="forward_stack",
    )(x, w1, w2)


def backward_kernel(tm, sub, per, len_ref, d_ref, h_ref, w1_ref, w2_ref, ds_ref, e_ref, dcur):
    step, m = pl.program_id(0), pl.program_id(1)
    last = pl.num_programs(0) - 1
    rows = pl.ds(pl.multiple_of(m * tm, tm), tm)

    def to_hidden():
        limit = len_ref[m // per] - (m % per) * tm
        keep = lax.broadcasted_iota(jnp.int32, (tm, d_ref.shape[-1]), 0) < limit
        fresh = jnp.where(keep, d_ref[...].astype(F32), 0.0).astype(BF16)
        ds_ref[0] = jnp.where(step == 0, fresh, dcur[rows, :])
        for s in range(w1_ref.shape[-1] // sub):
            cols = slice(s * sub, (s + 1) * sub)
            da = lax.dot_general(ds_ref[0], w2_ref[0, cols, :], NT, preferred_element_type=F32)
            e_ref[0, :, cols] = (da * gelu_tanh_grad(h_ref[0, :, cols].astype(F32))).astype(BF16)

    @pl.when(step < last)
    def _():
        to_hidden()
        for s in range(w2_ref.shape[-1] // sub):
            cols = slice(s * sub, (s + 1) * sub)
            back = lax.dot_general(e_ref[0], w1_ref[0, cols, :], NT, preferred_element_type=F32)
            dcur[rows, cols] = (ds_ref[0, :, cols].astype(F32) + back).astype(BF16)

    @pl.when(step == last)
    def _():
        to_hidden()


def backward_stack(lengths, d, h, w1, w2, seq, tm=512, sub=512):
    layers, dm, df = w1.shape
    m_rows = d.shape[0]
    nm = m_rows // tm
    return pl.pallas_call(
        functools.partial(backward_kernel, tm, sub, seq // tm),
        grid=(layers, nm),
        in_specs=[
            pl.BlockSpec(memory_space=pltpu.SMEM),
            pl.BlockSpec((tm, dm), lambda s, m: (jnp.where(s == 0, m, nm - 1), 0)),
            pl.BlockSpec((1, tm, df), lambda s, m: (layers - 1 - s, m, 0)),
            pl.BlockSpec((1, dm, df), lambda s, m: (jnp.maximum(layers - 1 - s, 1), 0, 0)),
            pl.BlockSpec((1, df, dm), lambda s, m: (layers - 1 - s, 0, 0)),
        ],
        out_specs=[
            pl.BlockSpec((1, tm, dm), lambda s, m: (layers - 1 - s, m, 0)),
            pl.BlockSpec((1, tm, df), lambda s, m: (layers - 1 - s, m, 0)),
        ],
        out_shape=[
            jax.ShapeDtypeStruct((layers, m_rows, dm), BF16),
            jax.ShapeDtypeStruct((layers, m_rows, df), BF16),
        ],
        scratch_shapes=[pltpu.VMEM((m_rows, dm), BF16)],
        compiler_params=params(2),
        name="backward_stack",
    )(lengths, d, h, w1, w2)


def fold(v):
    return jnp.sum(v.reshape(v.shape[0] // 8, 8, v.shape[1] // 128, 128), axis=(0, 2))


def gram_kernel(bs, x_ref, e_ref, a_ref, d_ref, o_ref):
    seq = x_ref.shape[0]
    once = jnp.zeros((8, 128), F32)
    twice = jnp.zeros((8, 128), F32)

    def block(ref, r0, r1, c0, c1):
        return lax.dot_general(ref[r0:r1, :], ref[c0:c1, :], NT, preferred_element_type=F32)

    for j in range(seq // bs):
        c0, c1 = j * bs, (j + 1) * bs
        for p, q in ((x_ref, e_ref), (d_ref, a_ref)):
            if j:
                twice += fold(block(p, 0, c0, c0, c1) * block(q, 0, c0, c0, c1))
            once += fold(block(p, c0, c1, c0, c1) * block(q, c0, c1, c0, c1))
    o_ref[0, 0] = once + 2.0 * twice


def gram_norms(x, e, a, d, seq, bs=256):
    layers, m_rows = x.shape[:2]
    return pl.pallas_call(
        functools.partial(gram_kernel, bs),
        grid=(layers, m_rows // seq),
        in_specs=[pl.BlockSpec((None, seq, v.shape[-1]), lambda l, i: (l, i, 0)) for v in (x, e, a, d)],
        out_specs=pl.BlockSpec((1, 1, 8, 128), lambda l, i: (l, i, 0, 0)),
        out_shape=jax.ShapeDtypeStruct((layers, m_rows // seq, 8, 128), F32),
        compiler_params=params(2),
        name="gram_norms",
    )(x, e, a, d)


TN = (((0,), (0,)), ((), ()))
MESH_ID = pl.DeviceIdType.MESH
SLOTS = 6
AG_SLOTS = 24
QUARTERS = 4
LAG = 3
STAGES = 8


def grad_sum_kernel(seq, n_chunks, factor_ref, xs_ref, a_ref, d_ref, e_ref, tot1_ref, tot2_ref,
                    lhs, raw, rhs, part, sum1, sum2, sum3, got0, got1, got2, got3, full,
                    load_sem, out_sem, send_sem, recv_sem):
    me = lax.axis_index("data")
    rows_all, width = rhs.shape
    tile = part.shape[1]
    core = me % 2
    sibling = me + 1 - 2 * core
    per_layer = 2 * QUARTERS

    def place(n):
        block = n // QUARTERS
        layer = block // per_layer
        return block, layer, block % per_layer

    def weight(color):
        return 2 + 2 * color + color * (color - 1)

    def route(color):
        w1, w2, w3 = weight(color), weight((color + 1) % 3), weight((color + 2) % 3)
        b1, b2, b3 = (me // w1) % 2, (me // w2) % 2, (me // w3) % 2
        n1, n2, n3 = me + w1 * (1 - 2 * b1), me + w2 * (1 - 2 * b2), me + w3 * (1 - 2 * b3)
        return (b1, b2, b3), (n1, n2, n3)

    barrier = pltpu.get_barrier_semaphore()
    _, near = route(0)
    for other in (sibling,) + near:
        pl.semaphore_signal(barrier, inc=1, device_id=(other,), device_id_type=MESH_ID)
    pl.semaphore_wait(barrier, 4)

    def aligned(v):
        return pl.multiple_of(v, 16)

    def loads(block, start):
        layer, which = block // per_layer, block % per_layer
        cols = pl.ds(pl.multiple_of((which % QUARTERS) * width, width), width)
        slot = block % 2

        def go(left, right):
            for copy in (pltpu.make_async_copy(left, lhs.at[slot], load_sem.at[0]),
                         pltpu.make_async_copy(right, raw, load_sem.at[1])):
                if start:
                    copy.start()
                else:
                    copy.wait()

        @pl.when(which < QUARTERS)
        def _():
            go(xs_ref.at[layer], e_ref.at[layer, :, cols])

        @pl.when(which >= QUARTERS)
        def _():
            go(a_ref.at[layer, :, cols], d_ref.at[layer])

    def remote(stage, n, src, dst, device):
        slot = n % SLOTS
        return pltpu.make_async_remote_copy(
            src_ref=src, dst_ref=dst, send_sem=send_sem.at[stage, slot], recv_sem=recv_sem.at[stage, slot],
            device_id=(device,), device_id_type=MESH_ID)

    def transfer(n, stage):
        slot, ag = n % SLOTS, n % AG_SLOTS
        (b1, b2, b3), (n1, n2, n3) = route(n % 3)
        half, quarter, eighth, piece = tile // 2, tile // 4, tile // 8, tile // 16

        def pick(ref, bit, size):
            return ref.at[slot, pl.ds(aligned((1 - bit) * size), size), :]

        def own(start, size):
            return full.at[ag, pl.ds(aligned(start), size), :]

        p1 = core * half
        p2 = p1 + b1 * quarter
        p3 = p2 + b2 * eighth
        p4 = p3 + b3 * piece
        if stage < 4:
            src, bit, size, got, device = ((part, core, half, got0, sibling), (sum1, b1, quarter, got1, n1),
                                           (sum2, b2, eighth, got2, n2), (sum3, b3, piece, got3, n3))[stage]
            return remote(stage, n, pick(src, bit, size), got.at[slot], device)
        start, size, device = ((p4, piece, n3), (p3, eighth, n2), (p2, quarter, n1), (p1, half, sibling))[stage - 4]
        return remote(stage, n, own(start, size), own(start, size), device)

    def add(n, stage):
        slot, ag = n % SLOTS, n % AG_SLOTS
        (b1, b2, b3), _ = route(n % 3)
        half, quarter, eighth, piece = tile // 2, tile // 4, tile // 8, tile // 16
        src, bit, size, got = ((part, core, half, got0), (sum1, b1, quarter, got1),
                               (sum2, b2, eighth, got2), (sum3, b3, piece, got3))[stage]
        value = (src[slot, pl.ds(aligned(bit * size), size), :].astype(F32) + got[slot].astype(F32)).astype(BF16)
        if stage < 3:
            (sum1, sum2, sum3)[stage][slot] = value
        else:
            full[ag, pl.ds(aligned(core * half + b1 * quarter + b2 * eighth + b3 * piece), piece), :] = value

    def out_copy(n, start):
        block, layer, which = place(n)
        ag, row = n % AG_SLOTS, (n % QUARTERS) * tile

        def go(dst):
            copy = pltpu.make_async_copy(full.at[ag], dst, out_sem.at[n % SLOTS])
            if start:
                copy.start()
            else:
                copy.wait()

        @pl.when(which < QUARTERS)
        def _():
            go(tot1_ref.at[layer, pl.ds(aligned(row), tile), pl.ds(pl.multiple_of((which % QUARTERS) * width, width), width)])

        @pl.when(which >= QUARTERS)
        def _():
            go(tot2_ref.at[layer, pl.ds(aligned((which % QUARTERS) * width + row), tile), :])

    def guarded(t, offset, fn):
        n = t - offset

        @pl.when((n >= 0) & (n < n_chunks))
        def _():
            fn(n)

    loads(0, True)
    first = 1
    done = first + STAGES * LAG

    def tick(t, carry):
        guarded(t, done + LAG, lambda n: out_copy(n, False))
        for stage in range(STAGES):
            def arrive(n, stage=stage):
                transfer(n, stage).wait()
                if stage < 4:
                    add(n, stage)
            guarded(t, first + LAG * (stage + 1), arrive)
        for stage in range(STAGES):
            guarded(t, first + LAG * stage, lambda n, stage=stage: transfer(n, stage).start())
        guarded(t, done, lambda n: out_copy(n, True))

        def compute(n):
            block = n // QUARTERS

            @pl.when(n % QUARTERS == 0)
            def _():
                loads(block, False)
                for i in range(rows_all // seq):
                    rhs[i * seq:(i + 1) * seq, :] = (raw[i * seq:(i + 1) * seq, :].astype(F32) * factor_ref[i]).astype(BF16)

                @pl.when(n + QUARTERS < n_chunks)
                def _():
                    loads(block + 1, True)

            cols = pl.ds(pl.multiple_of((n % QUARTERS) * tile, tile), tile)
            part[n % SLOTS] = lax.dot_general(lhs[block % 2, :, cols], rhs[...], TN, preferred_element_type=F32).astype(BF16)
        guarded(t, 0, compute)
        return carry

    lax.fori_loop(0, n_chunks + done + LAG, tick, 0)


def grad_sums(factor, xs, a, d, e, seq):
    layers, rows, dm = xs.shape
    df = a.shape[-1]
    tile = dm // QUARTERS
    n_chunks = layers * 2 * (df // dm) * QUARTERS
    hbm = pl.BlockSpec(memory_space=pl.ANY)

    def vmem(*shape):
        return pltpu.VMEM(shape, BF16)

    return pl.pallas_call(
        functools.partial(grad_sum_kernel, seq, n_chunks),
        in_specs=[pl.BlockSpec(memory_space=pltpu.SMEM), hbm, hbm, hbm, hbm],
        out_specs=[hbm, hbm],
        out_shape=[jax.ShapeDtypeStruct((layers, dm, df), BF16), jax.ShapeDtypeStruct((layers, df, dm), BF16)],
        scratch_shapes=[
            vmem(2, rows, dm), vmem(rows, dm), vmem(rows, dm),
            vmem(SLOTS, tile, dm), vmem(SLOTS, tile // 2, dm), vmem(SLOTS, tile // 4, dm), vmem(SLOTS, tile // 8, dm),
            vmem(SLOTS, tile // 2, dm), vmem(SLOTS, tile // 4, dm), vmem(SLOTS, tile // 8, dm), vmem(SLOTS, tile // 16, dm),
            vmem(AG_SLOTS, tile, dm),
            pltpu.SemaphoreType.DMA((2,)),
            pltpu.SemaphoreType.DMA((SLOTS,)),
            pltpu.SemaphoreType.DMA((STAGES, SLOTS)),
            pltpu.SemaphoreType.DMA((STAGES, SLOTS)),
        ],
        compiler_params=pltpu.CompilerParams(vmem_limit_bytes=VMEM_LIMIT, collective_id=0, has_side_effects=True),
        name="grad_sums",
    )(factor, xs, a, d, e)


def finish_kernel(scale, total_ref, noise_ref, out_ref):
    out_ref[...] = (total_ref[...].astype(F32) + noise_ref[...]) * scale


def finish(total, noise, scale):
    layers, rows, cols = noise.shape
    tile = (1 << 20) // cols
    return pl.pallas_call(
        functools.partial(finish_kernel, scale),
        grid=(layers, rows // tile),
        in_specs=[pl.BlockSpec((1, tile, cols), lambda l, r: (l, r, 0))] * 2,
        out_specs=pl.BlockSpec((1, tile, cols), lambda l, r: (l, r, 0)),
        out_shape=jax.ShapeDtypeStruct(noise.shape, F32),
        compiler_params=params(2),
        name="finish",
    )(total, noise)


def solution(mesh):
    devices = mesh.shape["data"]

    def body(x, dy, lengths, w1, w2, noise1, noise2, clip):
        samples, seq, dm = x.shape
        rows = samples * seq
        xs, h, a = forward_stack(x.reshape(rows, dm), w1, w2)
        d, e = backward_stack(lengths, dy.reshape(rows, dm), h, w1, w2, seq)
        norms = jnp.sum(gram_norms(xs, e, a, d, seq), axis=(0, 2, 3))
        factor = jnp.minimum(1.0, clip[0] / jnp.sqrt(norms))
        scale = 1.0 / (samples * devices)
        total1, total2 = grad_sums(factor, xs, a, d, e, seq)
        return finish(total1, noise1, scale), finish(total2, noise2, scale)

    data, whole = P("data"), P()
    return jax.shard_map(
        body,
        mesh=mesh,
        in_specs=(data, data, data, whole, whole, whole, whole, whole),
        out_specs=(whole, whole),
        check_vma=False,
    )
```

```python
import functools

import jax
import jax.numpy as jnp
from jax import lax
from jax.experimental import pallas as pl
from jax.experimental.pallas import tpu as pltpu
from jax.sharding import PartitionSpec as P

BF16 = jnp.bfloat16
F32 = jnp.float32
VMEM_LIMIT = 67_043_328
WINDOW = 512
C0 = 0.7978845608028654
C1 = 0.044715
NT = (((1,), (1,)), ((), ()))


def gelu_tanh(x):
    half = 0.5 * x
    return half + half * jnp.tanh(x * (C0 + (C0 * C1) * (x * x)))


def gelu_tanh_grad(x):
    sq = x * x
    t = jnp.tanh(x * (C0 + (C0 * C1) * sq))
    return (1.0 + t) * (0.5 + (x * (0.5 * C0 + (1.5 * C0 * C1) * sq)) * (1.0 - t))


def params(dims):
    return pltpu.CompilerParams(vmem_limit_bytes=VMEM_LIMIT, dimension_semantics=("arbitrary",) * dims)


def forward_kernel(tm, nu, nd, x_ref, *refs):
    w1 = refs[:nu]; w2 = refs[nu:nu + nd]
    xs_ref, h_ref, a_out, xcur, abuf, sem = refs[nu + nd:]
    layer, m = pl.program_id(0), pl.program_id(1)
    layers, nm = pl.num_programs(0), pl.num_programs(1)
    step = layer * nm + m
    slot = step % 2
    other = 1 - slot
    prev = step - 1

    def a_copy(s):
        return pltpu.make_async_copy(abuf.at[s % 2], a_out.at[s // nm, pl.ds(pl.multiple_of((s % nm) * tm, tm), tm), :], sem.at[s % 2])

    @pl.when(step >= 2)
    def _():
        a_copy(step - 2).wait()

    @pl.when(step >= 1)
    def _():
        a_copy(prev).start()

    rows = pl.ds(pl.multiple_of(m * tm, tm), tm)
    prow = pl.ds(pl.multiple_of((prev % nm) * tm, tm), tm)

    @pl.when(layer == 0)
    def _():
        xcur[rows, :] = x_ref[...]

    xs_ref[0] = xcur[rows, :]
    r = nu // nd

    def up(s):
        c = slice(s * WINDOW, (s + 1) * WINDOW)
        h_ref[0, :, c] = jnp.dot(xs_ref[0], w1[s][0], preferred_element_type=F32).astype(BF16)

    def act(c0, c1):
        abuf[slot, :, c0:c1] = gelu_tanh(h_ref[0, :, c0:c1].astype(F32)).astype(BF16)

    def down(s):
        c = slice(s * WINDOW, (s + 1) * WINDOW)
        branch = jnp.dot(abuf[other], w2[s][0], preferred_element_type=F32)
        xcur[prow, c] = (xcur[prow, c].astype(F32) + branch).astype(BF16)

    full = (step >= 1) & (prev < (layers - 1) * nm)

    @pl.when(full)
    def _():
        for s in range(nd):
            for q in range(r): up(s * r + q)
            down(s)
            act(s * r * WINDOW, (s + 1) * r * WINDOW)

    @pl.when(jnp.logical_not(full))
    def _():
        for s in range(nu):
            up(s)
            act(s * WINDOW, (s + 1) * WINDOW)

    @pl.when(step == layers * nm - 1)
    def _():
        a_copy(prev).wait()
        a_copy(step).start()
        a_copy(step).wait()

def forward_stack(x, w1, w2, tm=512):
    layers, dm, df = w1.shape
    m_rows = x.shape[0]
    nm = m_rows // tm
    nu, nd = df // WINDOW, dm // WINDOW

    def lag(l, m):
        return jnp.minimum(jnp.maximum(l * nm + m - 1, 0) // nm, layers - 2)

    return pl.pallas_call(
        functools.partial(forward_kernel, tm, nu, nd),
        grid=(layers, nm),
        in_specs=[pl.BlockSpec((tm, dm), lambda l, m: (jnp.where(l == 0, m, nm - 1), 0))]
        + [pl.BlockSpec((1, dm, WINDOW), lambda l, m, s=s: (l, 0, s)) for s in range(nu)]
        + [pl.BlockSpec((1, df, WINDOW), lambda l, m, s=s: (lag(l, m), 0, s)) for s in range(nd)],
        out_specs=[
            pl.BlockSpec((1, tm, dm), lambda l, m: (l, m, 0)),
            pl.BlockSpec((1, tm, df), lambda l, m: (l, m, 0)),
            pl.BlockSpec(memory_space=pl.ANY),
        ],
        out_shape=[
            jax.ShapeDtypeStruct((layers, m_rows, dm), BF16),
            jax.ShapeDtypeStruct((layers, m_rows, df), BF16),
            jax.ShapeDtypeStruct((layers, m_rows, df), BF16),
        ],
        scratch_shapes=[pltpu.VMEM((m_rows, dm), BF16), pltpu.VMEM((2, tm, df), BF16), pltpu.SemaphoreType.DMA((2,))],
        compiler_params=params(2),
        name="forward_stack",
    )(x, *([w1] * nu), *([w2] * nd))


def backward_kernel(tm, nu, nd, per, len_ref, d_ref, h_ref, *refs):
    w1 = refs[:nu]; w2 = refs[nu:nu + nd]
    ds_ref, e_ref, dcur = refs[nu + nd:]
    layer, m = pl.program_id(0), pl.program_id(1)
    last = pl.num_programs(0) - 1
    rows = pl.ds(pl.multiple_of(m * tm, tm), tm)
    dm = nd * WINDOW

    @pl.when(layer == 0)
    def _():
        limit = len_ref[m // per] - (m % per) * tm
        keep = lax.broadcasted_iota(jnp.int32, (tm, dm), 0) < limit
        dcur[rows, :] = jnp.where(keep, d_ref[...].astype(F32), 0.0).astype(BF16)

    ds_ref[0] = dcur[rows, :]

    def hidden(s):
        c = slice(s * WINDOW, (s + 1) * WINDOW)
        da = sum(lax.dot_general(ds_ref[0, :, k * WINDOW:(k + 1) * WINDOW], w2[k][0, c, :], NT, preferred_element_type=F32) for k in range(nd))
        e_ref[0, :, c] = (da * gelu_tanh_grad(h_ref[0, :, c].astype(F32))).astype(BF16)

    def back(s):
        c = slice(s * WINDOW, (s + 1) * WINDOW)
        v = sum(lax.dot_general(e_ref[0, :, k * WINDOW:(k + 1) * WINDOW], w1[k][0, c, :], NT, preferred_element_type=F32) for k in range(nu))
        dcur[rows, c] = (ds_ref[0, :, c].astype(F32) + v).astype(BF16)

    @pl.when(layer < last)
    def _():
        for s in range(nu): hidden(s)
        for s in range(nd): back(s)

    @pl.when(layer == last)
    def _():
        for s in range(nu): hidden(s)

def backward_stack(lengths, d, h, w1, w2, seq, tm=512):
    layers, dm, df = w1.shape
    m_rows = d.shape[0]
    nm = m_rows // tm
    nu, nd = df // WINDOW, dm // WINDOW
    return pl.pallas_call(
        functools.partial(backward_kernel, tm, nu, nd, seq // tm),
        grid=(layers, nm),
        in_specs=[
            pl.BlockSpec(memory_space=pltpu.SMEM),
            pl.BlockSpec((tm, dm), lambda s, m: (jnp.where(s == 0, m, nm - 1), 0)),
            pl.BlockSpec((1, tm, df), lambda s, m: (layers - 1 - s, m, 0)),
        ]
        + [pl.BlockSpec((1, dm, WINDOW), lambda s, m, k=k: (jnp.maximum(layers - 1 - s, 1), 0, k)) for k in range(nu)]
        + [pl.BlockSpec((1, df, WINDOW), lambda s, m, k=k: (layers - 1 - s, 0, k)) for k in range(nd)],
        out_specs=[
            pl.BlockSpec((1, tm, dm), lambda s, m: (layers - 1 - s, m, 0)),
            pl.BlockSpec((1, tm, df), lambda s, m: (layers - 1 - s, m, 0)),
        ],
        out_shape=[
            jax.ShapeDtypeStruct((layers, m_rows, dm), BF16),
            jax.ShapeDtypeStruct((layers, m_rows, df), BF16),
        ],
        scratch_shapes=[pltpu.VMEM((m_rows, dm), BF16)],
        compiler_params=params(2),
        name="backward_stack",
    )(lengths, d, h, *([w1] * nu), *([w2] * nd))


def fold(v):
    return jnp.sum(v.reshape(v.shape[0] // 8, 8, v.shape[1] // 128, 128), axis=(0, 2))


def gram_kernel(bs, x_ref, e_ref, a_ref, d_ref, o_ref):
    seq = x_ref.shape[0]
    once = jnp.zeros((8, 128), F32)
    twice = jnp.zeros((8, 128), F32)

    def block(ref, r0, r1, c0, c1):
        return lax.dot_general(ref[r0:r1, :], ref[c0:c1, :], NT, preferred_element_type=F32)

    for j in range(seq // bs):
        c0, c1 = j * bs, (j + 1) * bs
        for p, q in ((x_ref, e_ref), (d_ref, a_ref)):
            if j:
                twice += fold(block(p, 0, c0, c0, c1) * block(q, 0, c0, c0, c1))
            once += fold(block(p, c0, c1, c0, c1) * block(q, c0, c1, c0, c1))
    o_ref[0, 0] = once + 2.0 * twice


def gram_norms(x, e, a, d, seq, bs=256):
    layers, m_rows = x.shape[:2]
    return pl.pallas_call(
        functools.partial(gram_kernel, bs),
        grid=(layers, m_rows // seq),
        in_specs=[pl.BlockSpec((None, seq, v.shape[-1]), lambda l, i: (l, i, 0)) for v in (x, e, a, d)],
        out_specs=pl.BlockSpec((1, 1, 8, 128), lambda l, i: (l, i, 0, 0)),
        out_shape=jax.ShapeDtypeStruct((layers, m_rows // seq, 8, 128), F32),
        compiler_params=params(2),
        name="gram_norms",
    )(x, e, a, d)


TN = (((0,), (0,)), ((), ()))
MESH_ID = pl.DeviceIdType.MESH
SLOTS = 6
AG_SLOTS = 24
QUARTERS = 4
LAG = 3
STAGES = 8
NOISE_SLOTS = 9


def grad_sum_kernel(seq, n_chunks, scale, factor_ref, xs_ref, a_ref, d_ref, e_ref, noise1_ref, noise2_ref, out1_ref, out2_ref,
                    lhs, raw, rhs, part, sum1, sum2, sum3, got0, got1, got2, got3, full, final,
                    load_sem, noise_sem, out_sem, send_sem, recv_sem):
    me = lax.axis_index("data")
    rows_all, width = rhs.shape
    tile = part.shape[1]
    core = me % 2
    sibling = me + 1 - 2 * core
    per_layer = 2 * QUARTERS

    def place(n):
        block = n // QUARTERS
        layer = block // per_layer
        return block, layer, block % per_layer

    def weight(color):
        return 2 + 2 * color + color * (color - 1)

    def route(color):
        w1, w2, w3 = weight(color), weight((color + 1) % 3), weight((color + 2) % 3)
        b1, b2, b3 = (me // w1) % 2, (me // w2) % 2, (me // w3) % 2
        n1, n2, n3 = me + w1 * (1 - 2 * b1), me + w2 * (1 - 2 * b2), me + w3 * (1 - 2 * b3)
        return (b1, b2, b3), (n1, n2, n3)

    barrier = pltpu.get_barrier_semaphore()
    _, near = route(0)
    for other in (sibling,) + near:
        pl.semaphore_signal(barrier, inc=1, device_id=(other,), device_id_type=MESH_ID)
    pl.semaphore_wait(barrier, 4)

    def aligned(v):
        return pl.multiple_of(v, 16)

    def loads(block, start):
        layer, which = block // per_layer, block % per_layer
        cols = pl.ds(pl.multiple_of((which % QUARTERS) * width, width), width)
        slot = block % 2

        def go(left, right):
            for copy in (pltpu.make_async_copy(left, lhs.at[slot], load_sem.at[0]),
                         pltpu.make_async_copy(right, raw, load_sem.at[1])):
                if start:
                    copy.start()
                else:
                    copy.wait()

        @pl.when(which < QUARTERS)
        def _():
            go(xs_ref.at[layer], e_ref.at[layer, :, cols])

        @pl.when(which >= QUARTERS)
        def _():
            go(a_ref.at[layer, :, cols], d_ref.at[layer])

    def remote(stage, n, src, dst, device):
        slot = n % SLOTS
        return pltpu.make_async_remote_copy(
            src_ref=src, dst_ref=dst, send_sem=send_sem.at[stage, slot], recv_sem=recv_sem.at[stage, slot],
            device_id=(device,), device_id_type=MESH_ID)

    def transfer(n, stage):
        slot, ag = n % SLOTS, n % AG_SLOTS
        (b1, b2, b3), (n1, n2, n3) = route(n % 3)
        half, quarter, eighth, piece = tile // 2, tile // 4, tile // 8, tile // 16

        def pick(ref, bit, size):
            return ref.at[slot, pl.ds(aligned((1 - bit) * size), size), :]

        def own(start, size):
            return full.at[ag, pl.ds(aligned(start), size), :]

        p1 = core * half
        p2 = p1 + b1 * quarter
        p3 = p2 + b2 * eighth
        p4 = p3 + b3 * piece
        if stage < 4:
            src, bit, size, got, device = ((part, core, half, got0, sibling), (sum1, b1, quarter, got1, n1),
                                           (sum2, b2, eighth, got2, n2), (sum3, b3, piece, got3, n3))[stage]
            return remote(stage, n, pick(src, bit, size), got.at[slot], device)
        start, size, device = ((p4, piece, n3), (p3, eighth, n2), (p2, quarter, n1), (p1, half, sibling))[stage - 4]
        return remote(stage, n, own(start, size), own(start, size), device)

    def add(n, stage):
        slot, ag = n % SLOTS, n % AG_SLOTS
        (b1, b2, b3), _ = route(n % 3)
        half, quarter, eighth, piece = tile // 2, tile // 4, tile // 8, tile // 16
        src, bit, size, got = ((part, core, half, got0), (sum1, b1, quarter, got1),
                               (sum2, b2, eighth, got2), (sum3, b3, piece, got3))[stage]
        value = (src[slot, pl.ds(aligned(bit * size), size), :].astype(F32) + got[slot].astype(F32)).astype(BF16)
        if stage < 3:
            (sum1, sum2, sum3)[stage][slot] = value
        else:
            full[ag, pl.ds(aligned(core * half + b1 * quarter + b2 * eighth + b3 * piece), piece), :] = value

    def final_copy(n, inward, start):
        _, layer, which = place(n)
        slot, row = n % NOISE_SLOTS, (n % QUARTERS) * tile

        def go(ref):
            if inward:
                copy = pltpu.make_async_copy(ref, final.at[slot], noise_sem.at[slot])
            else:
                copy = pltpu.make_async_copy(final.at[slot], ref, out_sem.at[slot])
            if start:
                copy.start()
            else:
                copy.wait()

        @pl.when(which < QUARTERS)
        def _():
            ref = noise1_ref if inward else out1_ref
            go(ref.at[layer, pl.ds(aligned(row), tile), pl.ds(pl.multiple_of((which % QUARTERS) * width, width), width)])

        @pl.when(which >= QUARTERS)
        def _():
            ref = noise2_ref if inward else out2_ref
            go(ref.at[layer, pl.ds(aligned((which % QUARTERS) * width + row), tile), :])

    def finish(n):
        final_copy(n, True, False)
        slot = n % NOISE_SLOTS
        final[slot] = (full[n % AG_SLOTS].astype(F32) + final[slot]) * scale

    def guarded(t, offset, fn):
        n = t - offset

        @pl.when((n >= 0) & (n < n_chunks))
        def _():
            fn(n)

    loads(0, True)
    first = 1
    done = first + STAGES * LAG

    def tick(t, carry):
        guarded(t, done + LAG, lambda n: final_copy(n, False, False))
        for stage in range(STAGES):
            def arrive(n, stage=stage):
                transfer(n, stage).wait()
                if stage < 4:
                    add(n, stage)
            guarded(t, first + LAG * (stage + 1), arrive)
        for stage in range(STAGES):
            guarded(t, first + LAG * stage, lambda n, stage=stage: transfer(n, stage).start())
        guarded(t, done, finish)
        guarded(t, done - LAG, lambda n: final_copy(n, True, True))

        def compute(n):
            block = n // QUARTERS

            @pl.when(n % QUARTERS == 0)
            def _():
                loads(block, False)
                for i in range(rows_all // seq):
                    rhs[i * seq:(i + 1) * seq, :] = (raw[i * seq:(i + 1) * seq, :].astype(F32) * factor_ref[i]).astype(BF16)

                @pl.when(n + QUARTERS < n_chunks)
                def _():
                    loads(block + 1, True)

            cols = pl.ds(pl.multiple_of((n % QUARTERS) * tile, tile), tile)
            part[n % SLOTS] = lax.dot_general(lhs[block % 2, :, cols], rhs[...], TN, preferred_element_type=F32).astype(BF16)
        guarded(t, 0, compute)
        guarded(t, done, lambda n: final_copy(n, False, True))
        return carry

    lax.fori_loop(0, n_chunks + done + LAG, tick, 0)


def grad_sums(factor, xs, a, d, e, noise1, noise2, seq, scale):
    layers, rows, dm = xs.shape
    df = a.shape[-1]
    tile = dm // QUARTERS
    n_chunks = layers * 2 * (df // dm) * QUARTERS
    hbm = pl.BlockSpec(memory_space=pl.ANY)

    def vmem(*shape):
        return pltpu.VMEM(shape, BF16)

    return pl.pallas_call(
        functools.partial(grad_sum_kernel, seq, n_chunks, scale),
        in_specs=[pl.BlockSpec(memory_space=pltpu.SMEM)] + [hbm] * 6,
        out_specs=[hbm, hbm],
        out_shape=[jax.ShapeDtypeStruct((layers, dm, df), F32), jax.ShapeDtypeStruct((layers, df, dm), F32)],
        scratch_shapes=[
            vmem(2, rows, dm), vmem(rows, dm), vmem(rows, dm),
            vmem(SLOTS, tile, dm), vmem(SLOTS, tile // 2, dm), vmem(SLOTS, tile // 4, dm), vmem(SLOTS, tile // 8, dm),
            vmem(SLOTS, tile // 2, dm), vmem(SLOTS, tile // 4, dm), vmem(SLOTS, tile // 8, dm), vmem(SLOTS, tile // 16, dm),
            vmem(AG_SLOTS, tile, dm),
            pltpu.VMEM((NOISE_SLOTS, tile, dm), F32),
            pltpu.SemaphoreType.DMA((2,)),
            pltpu.SemaphoreType.DMA((NOISE_SLOTS,)),
            pltpu.SemaphoreType.DMA((NOISE_SLOTS,)),
            pltpu.SemaphoreType.DMA((STAGES, SLOTS)),
            pltpu.SemaphoreType.DMA((STAGES, SLOTS)),
        ],
        compiler_params=pltpu.CompilerParams(vmem_limit_bytes=VMEM_LIMIT, collective_id=0, has_side_effects=True),
        name="grad_sums",
    )(factor, xs, a, d, e, noise1, noise2)


def hand_over_kernel(src_ref, dst_ref):
    dst_ref[...] = src_ref[...]


def hand_over(v):
    layers, rows, cols = v.shape
    tile = (1 << 20) // cols
    spec = pl.BlockSpec((1, tile, cols), lambda l, r: (l, r, 0))
    return pl.pallas_call(
        hand_over_kernel,
        grid=(layers, rows // tile),
        in_specs=[spec],
        out_specs=spec,
        out_shape=jax.ShapeDtypeStruct(v.shape, v.dtype),
        compiler_params=params(2),
        name="hand_over",
    )(v)


def solution(mesh):
    devices = mesh.shape["data"]

    def body(x, dy, lengths, w1, w2, noise1, noise2, clip):
        samples, seq, dm = x.shape
        rows = samples * seq
        xs, h, a = forward_stack(x.reshape(rows, dm), w1, w2)
        d, e = backward_stack(lengths, dy.reshape(rows, dm), h, w1, w2, seq)
        norms = jnp.sum(gram_norms(xs, e, a, d, seq), axis=(0, 2, 3))
        factor = jnp.minimum(1.0, clip[0] / jnp.sqrt(norms))
        out1, out2 = grad_sums(factor, xs, a, d, e, noise1, noise2, seq, 1.0 / (samples * devices))
        return hand_over(out1), hand_over(out2)

    data, whole = P("data"), P()
    return jax.shard_map(
        body,
        mesh=mesh,
        in_specs=(data, data, data, whole, whole, whole, whole, whole),
        out_specs=(whole, whole),
        check_vma=False,
    )
```
